32 devices in a mesh: head: 4 (over z), batch: 8 (over y, x, core).
Axes of the slice: x: 2, y: 2, z: 4, core: 2. Of those that a mesh axis runs over, the one named last changes fastest.
Arguments:
- window_ids: int32 [32, 22], replicated, may hold values from 0 to 64127
- pool_ids: int32 [32, 64, 3], replicated, may hold values from 0 to 64127
- guess_index: int32 [32, 7], replicated, may hold values from 0 to 63
- lengths: int32 [32], P('batch'), may hold values from 16 to 2048, as said below
- embed_table: bfloat16 [64128, 8192], P('batch', 'head'), may hold values from -6 to 6
- w_query: bfloat16 [8192, 8192], P('batch', 'head'), may hold values from -0.0625 to 0.0625
- w_key: bfloat16 [8192, 1024], P('batch', 'head'), may hold values from -0.0625 to 0.0625
- w_value: bfloat16 [8192, 1024], P('batch', 'head'), may hold values from -0.0625 to 0.0625
- k_cache: bfloat16 [8, 32, 2048, 128], P(None, None, ('head', 'batch')), may hold values from -300 to 300
- v_cache: bfloat16 [8, 32, 2048, 128], P(None, None, ('head', 'batch')), may hold values from -12 to 12
Outputs:
- attended: bfloat16 [1376, 8192], P('batch', 'head')
- k_decode: bfloat16 [8, 32, 2048, 128], P('head', 'batch')
- v_decode: bfloat16 [8, 32, 2048, 128], P('head', 'batch')
The draws below stay inside these ranges and needn't reach their ends.
Inputs may be any that keep to these rules, and one draw needn't show every extreme that they name: `lengths`: in every draw one sequence has exactly 2048 cached tokens.
All inputs are finite; a program needn't handle non-finite values.
Results may differ from the reference program's by a relative error of at most 0.0055.
The reference program's roundings to bfloat16 on the way (of `embedded`, `normed`, `queries`, `keys_new`, `values_new` and `weights`) count: a program that leaves them out, or rounds other values in their place, can miss the bound.
Values may be sent and summed in bfloat16 or wider, within the bound.
No kernel may reach another device: no remote copies, remote signals or barrier semaphores. Data moves between devices by JAX's collectives and lax.ppermute only.
A program may use at most 192 MiB of HBM per device.

```python
import math
import jax
import jax.numpy as jnp
import numpy as np
from jax import lax

D = 8192
QH = 64
KVH = 8
HD = 128
VOCAB = 64128
W = 7
NG = 4
G = 7
POOL = 64
CTX = 2048
SEQS = 32


def draw_lengths(key, part):
    top_power = CTX.bit_length() - 1
    power_key = jax.random.fold_in(key, 3)
    extra_key = jax.random.fold_in(key, 5)
    chosen_key = jax.random.fold_in(key, 7)
    powers = jax.random.randint(power_key, (SEQS,), 4, top_power)
    base_len = jnp.left_shift(jnp.ones((SEQS,), jnp.int32), powers.astype(jnp.int32))
    extra_len = jax.random.randint(extra_key, (SEQS,), 0, base_len)
    drawn_len = base_len + extra_len
    chosen = jax.random.randint(chosen_key, (), 0, SEQS)
    return jnp.where(jnp.arange(SEQS) == chosen, CTX, drawn_len).astype(jnp.int32)


def draw_k_cache(key, part):
    normal_part = 2.0 * jax.random.normal(jax.random.fold_in(key, 11), (KVH, SEQS, CTX, HD), jnp.float32)
    return jnp.clip(normal_part, -300.0, 300.0).astype(jnp.bfloat16)


def plant(result, rng, smallest, top_value):
    longest = result.shape.index(max(result.shape))
    spots = []
    for shift in (0, 1):
        where = [jax.random.randint(jax.random.fold_in(rng, axis), (), 0, length) for axis, length in enumerate(result.shape)]
        where[longest] = (where[longest] + shift) % result.shape[longest]
        spots.append(tuple(where))
    return result.at[spots[0]].set(smallest).at[spots[1]].set(top_value)


def block_levels(rng, dims, split, least, top_value):
    factor_of, own = 1.0, jax.random.fold_in(rng, 6)
    for axis_at, blocks in split:
        steps = jnp.exp(jax.random.uniform(jax.random.fold_in(own, axis_at), (blocks,), jnp.float32, least / len(split), top_value / len(split)))
        factor_of = factor_of * jnp.repeat(steps, dims[axis_at] // blocks).reshape([-1 if axis == axis_at else 1 for axis in range(len(dims))])
    return factor_of


def rank_bounds(amount, lean):
    loads = [(1 << 20) // math.isqrt(standing ** lean) + 1 for standing in range(1, amount + 1)]
    deviation = 1 + sum(loads) // (1 << 30)
    return np.cumsum(np.array([max(1, weight // deviation) for weight in loads]))


def skewed_ids(own_key, extent, count, skew):
    table = rank_bounds(count, skew)
    lot = jax.random.randint(jax.random.fold_in(own_key, 1), extent, 0, int(table[count - 1]))
    standing = jnp.searchsorted(jnp.asarray(table, jnp.int32), lot, side="right")
    return jax.random.permutation(jax.random.fold_in(own_key, 2), count)[standing].astype(jnp.int32)


def bell_draw(key, dims, deviation, bound, split=(), kind=jnp.bfloat16):
    gain = block_levels(key, dims, split, -0.22, 0.18) if split else 1.0
    drawn = jax.random.normal(key, dims, jnp.float32) * deviation * gain
    return jnp.minimum(jnp.maximum(drawn, -bound), bound).astype(kind)


def setup_inputs(seed: int = 0) -> dict:
    seeds = jax.random.split(jax.random.key(seed), 11)
    return {
        "window_ids": plant(skewed_ids(seeds[0], (SEQS, 1 + (NG - 1) * W), VOCAB, 2), jax.random.fold_in(seeds[0], 3), 0, VOCAB - 1).astype(jnp.int32),
        "pool_ids": plant(skewed_ids(seeds[1], (SEQS, POOL, NG - 1), VOCAB, 2), jax.random.fold_in(seeds[1], 3), 0, VOCAB - 1).astype(jnp.int32),
        "guess_index": plant(jax.random.randint(seeds[2], (SEQS, G), 0, POOL), jax.random.fold_in(seeds[2], 1), 0, POOL - 1).astype(jnp.int32),
        "lengths": draw_lengths(jax.random.fold_in(seeds[10], 71), 0),
        "embed_table": bell_draw(seeds[4], (VOCAB, D), 1.0, 6.0, ((0, 8), (1, 4))),
        "w_query": bell_draw(seeds[5], (D, QH * HD), D ** -0.5, 0.0625, ((0, 8), (1, 4))),
        "w_key": bell_draw(seeds[6], (D, KVH * HD), D ** -0.5, 0.0625, ((0, 8), (1, 4))),
        "w_value": bell_draw(seeds[7], (D, KVH * HD), D ** -0.5, 0.0625, ((0, 8), (1, 4))),
        "k_cache": draw_k_cache(jax.random.fold_in(seeds[10], 71), 0),
        "v_cache": bell_draw(seeds[9], (KVH, SEQS, CTX, HD), 2.0, 12.0, ((2, 32),)),
    }


ROPE_BASE = 500000.0
NORM_EPS = 1e-05

def layout_tables():
    levels = NG - 1
    level_of = np.repeat(np.arange(levels), W)
    column_of = np.tile(np.arange(W), levels)
    window_mask = (level_of[None, :] == 0) & (column_of[None, :] <= column_of[:, None]) | (column_of[None, :] == column_of[:, None]) & (level_of[None, :] <= level_of[:, None])
    guess_of = np.repeat(np.arange(G), levels)
    slot_of = np.tile(np.arange(levels), G)
    guess_mask = (guess_of[None, :] == guess_of[:, None]) & (slot_of[None, :] <= slot_of[:, None])
    window_rows = levels * W
    total_rows = 1 + window_rows + G * levels
    allowed = np.zeros((total_rows, total_rows), np.bool_)
    allowed[:, 0] = True
    allowed[1:1 + window_rows, 1:1 + window_rows] = window_mask
    allowed[1 + window_rows:, 1 + window_rows:] = guess_mask
    offsets = np.concatenate([np.zeros(1, np.int32), (1 + level_of + column_of).astype(np.int32), (1 + slot_of).astype(np.int32)])
    return (offsets, allowed)

def gather_ids(window_ids, pool_ids, guess_index):
    wanted = jnp.broadcast_to(guess_index[:, :, None], (guess_index.shape[0], guess_index.shape[1], pool_ids.shape[2])).astype(jnp.int32)
    picked = jnp.take_along_axis(pool_ids, wanted, axis=1)
    return jnp.concatenate([window_ids, picked.reshape(picked.shape[0], -1)], axis=1)

def rotate(vectors, positions):
    head_dim = vectors.shape[-1]
    half_dim = head_dim // 2
    ladder = jnp.arange(half_dim).astype(jnp.float32)
    frequencies = jnp.power(ROPE_BASE, ladder * (-2.0 / head_dim))
    angles = positions.astype(jnp.float32)[..., None] * frequencies
    cosine = jnp.cos(angles)[..., None, :]
    sines = jnp.sin(angles)[..., None, :]
    front_half = vectors[..., :half_dim]
    second = vectors[..., half_dim:]
    return jnp.concatenate([front_half * cosine - second * sines, second * cosine + front_half * sines], axis=-1)

def reference(window_ids, pool_ids, guess_index, lengths, embed_table, w_query, w_key, w_value, k_cache, v_cache):
    offsets, allowed = layout_tables()
    total_rows = offsets.shape[0]
    per_group = QH // KVH
    token_ids = gather_ids(window_ids, pool_ids, guess_index)
    embedded = jnp.take(embed_table, token_ids.reshape(-1), axis=0).astype(jnp.float32)
    normed = (embedded * lax.rsqrt(lax.optimization_barrier(jnp.mean(embedded * embedded, axis=-1, keepdims=True)) + NORM_EPS)).astype(jnp.bfloat16)
    query_raw = jnp.dot(normed, w_query, preferred_element_type=jnp.float32)
    key_raw = jnp.dot(normed, w_key, preferred_element_type=jnp.float32)
    value_raw = jnp.dot(normed, w_value, preferred_element_type=jnp.float32)
    positions = lengths[:, None] + jnp.asarray(offsets).astype(jnp.int32)[None, :]
    queries = rotate(query_raw.reshape(SEQS, total_rows, QH, HD), positions).astype(jnp.bfloat16)
    keys_new = rotate(key_raw.reshape(SEQS, total_rows, KVH, HD), positions).astype(jnp.bfloat16)
    values_new = value_raw.astype(jnp.bfloat16).reshape(SEQS, total_rows, KVH, HD)
    causal = jnp.asarray(allowed)
    score_scale = HD ** (-0.5)

    def one_sequence(operands):
        q_seq, k_seq, v_seq, k_old, v_old, length = operands
        q_five = q_seq.reshape(total_rows, KVH, per_group, HD).astype(jnp.float32)
        keys_all = jnp.concatenate([k_old, jnp.swapaxes(k_seq, 0, 1)], axis=1).astype(jnp.float32)
        values_all = jnp.concatenate([v_old, jnp.swapaxes(v_seq, 0, 1)], axis=1).astype(jnp.float32)
        scores = jnp.einsum('tkgd,kcd->kgtc', q_five, keys_all) * score_scale
        visible = jnp.concatenate([jnp.broadcast_to((jnp.arange(CTX) < length)[None, :], (total_rows, CTX)), causal], axis=1)
        scores = jnp.where(visible, scores, -1e+30)
        row_peak = lax.optimization_barrier(jnp.max(scores, axis=-1, keepdims=True))
        powers = jnp.exp(scores - row_peak)
        weights = (powers / lax.optimization_barrier(jnp.sum(powers, axis=-1, keepdims=True))).astype(jnp.bfloat16)
        blended = jnp.einsum('kgtc,kcd->tkgd', weights.astype(jnp.float32), values_all)
        return blended.reshape(total_rows, QH * HD).astype(jnp.bfloat16)
    attended = lax.map(one_sequence, (queries, keys_new, values_new, jnp.swapaxes(k_cache, 0, 1), jnp.swapaxes(v_cache, 0, 1), lengths))
    return (attended.reshape(SEQS * total_rows, QH * HD), k_cache, v_cache)
```

```python
import jax
import jax.numpy as jnp
import numpy as np
from jax import lax
from jax.experimental import pallas as pl
from jax.experimental.pallas import tpu as pltpu
from jax.sharding import PartitionSpec as P


W = 7
NG = 4
G = 7

ROPE_BASE = 500000.0
NORM_EPS = 1e-05
SLOTS = 32
UNROLL = 4
CHUNK = 512
SUM_TYPE = jnp.float16


def layout_tables():
    levels = NG - 1
    level_of = np.repeat(np.arange(levels), W)
    column_of = np.tile(np.arange(W), levels)
    window_mask = (level_of[None, :] == 0) & (column_of[None, :] <= column_of[:, None]) | (
        column_of[None, :] == column_of[:, None]
    ) & (level_of[None, :] <= level_of[:, None])
    guess_of = np.repeat(np.arange(G), levels)
    slot_of = np.tile(np.arange(levels), G)
    guess_mask = (guess_of[None, :] == guess_of[:, None]) & (slot_of[None, :] <= slot_of[:, None])
    window_rows = levels * W
    total_rows = 1 + window_rows + G * levels
    allowed = np.zeros((total_rows, total_rows), np.bool_)
    allowed[:, 0] = True
    allowed[1 : 1 + window_rows, 1 : 1 + window_rows] = window_mask
    allowed[1 + window_rows :, 1 + window_rows :] = guess_mask
    offsets = np.concatenate(
        [
            np.zeros(1, np.int32),
            (1 + level_of + column_of).astype(np.int32),
            (1 + slot_of).astype(np.int32),
        ]
    )
    return (offsets, allowed)


def round_up(value, unit):
    return -(-value // unit) * unit


def lookup_rows(window_ids, pool_ids, guess_index, embed_table, n_batch, rows_seq):
    seqs, window = window_ids.shape
    guesses = guess_index.shape[1]
    pool, levels = pool_ids.shape[1:]
    seq_dev = seqs // n_batch
    vocab_rows, width = embed_table.shape
    group_rows = seq_dev * rows_seq
    half = (n_batch // 2) * group_rows
    table = embed_table.reshape(vocab_rows // 8, 8, width)
    most = n_batch * group_rows

    def kernel(me_ref, window_ref, pool_ref, guess_ref, table_ref, even_ref, odd_ref, rows, held, where_to, which, sems):
        me = me_ref[0]
        first = me * vocab_rows

        def clear(i, _):
            rows[pl.ds(pl.multiple_of(i * 8, 8), 8), :] = jnp.zeros((8, width), jnp.float32)
            return 0

        lax.fori_loop(0, most // 8, clear, 0)

        def note(token, row, found):
            local = token - first
            where_to[found] = row
            which[found] = local
            return found + jnp.where(jnp.logical_and(local >= 0, local < vocab_rows), 1, 0)

        def scan(seq, found):
            step = jnp.bitwise_xor(seq // seq_dev, me)
            place = (step % 2) * (n_batch // 2) + step // 2
            base = place * group_rows + (seq % seq_dev) * rows_seq
            for i in range(window):
                found = note(window_ref[seq, i], base + i, found)
            for g in range(guesses):
                at = guess_ref[seq, g] * levels
                for j in range(levels):
                    found = note(pool_ref[seq, at + j], base + window + g * levels + j, found)
            return found

        found = lax.fori_loop(0, seqs, scan, 0)

        for n in range(UNROLL):
            where_to[found + n] = most
            which[found + n] = 0
        groups = (found + UNROLL - 1) // UNROLL

        def fetch(i, slot):
            return pltpu.make_async_copy(
                table_ref.at[lax.shift_right_logical(which[i], 3)], held.at[slot], sems.at[slot]
            )

        def prime(i, _):
            for n in range(UNROLL):
                fetch(i * UNROLL + n, i * UNROLL + n).start()
            return 0

        lax.fori_loop(0, jnp.minimum(groups, SLOTS // UNROLL), prime, 0)
        sub = lax.broadcasted_iota(jnp.int32, (8, width), 0)

        def take(i, _):
            slot = lax.rem(i, SLOTS // UNROLL) * UNROLL
            for n in range(UNROLL):
                fetch(i * UNROLL + n, slot + n).wait()
            for n in range(UNROLL):
                source, target = which[i * UNROLL + n], where_to[i * UNROLL + n]
                low = jnp.bitwise_and(target, 7)
                tile = held[slot + n].astype(jnp.float32)
                turned = pltpu.roll(tile, jnp.bitwise_and(low - source, 7), 0)
                at = pl.ds(pl.multiple_of(target - low, 8), 8)
                rows[at, :] = jnp.where(sub == low, turned, rows[at, :])

            @pl.when(i + SLOTS // UNROLL < groups)
            def _():
                for n in range(UNROLL):
                    fetch((i + SLOTS // UNROLL) * UNROLL + n, slot + n).start()

            return 0

        lax.fori_loop(0, groups, take, 0)

        def narrow(i, _):
            at = pl.multiple_of(i * 16, 16)
            even_ref[pl.ds(at, 16), :] = rows[pl.ds(at, 16), :].astype(jnp.bfloat16)
            odd_ref[pl.ds(at, 16), :] = rows[pl.ds(at + half, 16), :].astype(jnp.bfloat16)
            return 0

        lax.fori_loop(0, half // 16, narrow, 0)

    smem = pl.BlockSpec(memory_space=pltpu.SMEM)
    vmem = pl.BlockSpec(memory_space=pltpu.VMEM)
    out = jax.ShapeDtypeStruct((half, width), jnp.bfloat16)
    me = lax.axis_index("batch").astype(jnp.int32).reshape(1)
    even, odd = pl.pallas_call(
        kernel,
        out_shape=(out, out),
        in_specs=[smem, smem, smem, smem, pl.BlockSpec(memory_space=pltpu.HBM)],
        out_specs=(vmem, vmem),
        scratch_shapes=[
            pltpu.VMEM((most + 8, width), jnp.float32),
            pltpu.VMEM((SLOTS, 8, width), jnp.bfloat16),
            pltpu.SMEM((most + 8,), jnp.int32),
            pltpu.SMEM((most + 8,), jnp.int32),
            pltpu.SemaphoreType.DMA((SLOTS,)),
        ],
        cost_estimate=pl.CostEstimate(flops=10_000_000_000, bytes_accessed=20_000_000, transcendentals=0),
        name="lookup",
    )(me, window_ids, pool_ids.reshape(seqs, pool * levels), guess_index, table)
    shape = (n_batch // 2, group_rows, width)
    return even.reshape(shape), odd.reshape(shape)


def score_head(k, qkv, visible_new, lengths, k_got, kv_dev, per_group, earlier):
    senders, seq_dev, slab, head_dim = k_got.shape
    context = senders * slab
    chunk = min(CHUNK, context)
    chunks = context // chunk
    part = chunk // slab
    rows_pad = qkv.shape[1]
    rows = per_group * rows_pad
    q_cols = per_group * head_dim
    scale = head_dim ** (-0.5)
    f32, bf16 = jnp.float32, jnp.bfloat16
    dims = (((1,), (1,)), ((), ()))
    plain = (((1,), (0,)), ((), ()))

    def kernel(len_ref, q_ref, kn_ref, vn_ref, mask_ref, k_ref, *refs):
        w_ref, new_ref, ko_ref, q_all, score, peak, total = refs[-7:]
        length = len_ref[pl.program_id(0)]
        for g in range(per_group):
            q_all[pl.ds(g * rows_pad, rows_pad), :] = q_ref[0, :, pl.ds(g * head_dim, head_dim)]
        k_new, v_new = kn_ref[0], vn_ref[0]
        s_new = lax.dot_general(q_all[...], k_new, dims, preferred_element_type=f32) * scale
        s_new = jnp.where(mask_ref[...] > 0, s_new, -1e30)
        peak[...] = jnp.max(s_new, axis=-1, keepdims=True)
        for i in range(chunks):
            ko_ref[0, 0, pl.ds(i * chunk, chunk), :] = k_ref[pl.ds(i * part, part), 0].reshape(chunk, head_dim)

        for i in range(chunks):

            @pl.when(i * chunk < length)
            def _(i=i):
                got = lax.dot_general(
                    q_all[...], ko_ref[0, 0, pl.ds(i * chunk, chunk), :], dims, preferred_element_type=f32
                ) * scale
                at = lax.broadcasted_iota(jnp.int32, (rows, chunk), 1) + i * chunk
                got = jnp.where(at < length, got, -1e30)
                score[i] = got
                peak[...] = jnp.maximum(peak[...], jnp.max(got, axis=-1, keepdims=True))

        p_new = jnp.exp(s_new - peak[...])
        total[...] = jnp.sum(p_new, axis=-1, keepdims=True)
        for i in range(chunks):

            @pl.when(i * chunk < length)
            def _(i=i):
                p = jnp.exp(score[i] - peak[...])
                score[i] = p
                total[...] += jnp.sum(p, axis=-1, keepdims=True)

        inverse = 1.0 / total[...]
        new_ref[0] = lax.dot_general((p_new * inverse).astype(bf16), v_new, plain, preferred_element_type=f32)
        for i in range(chunks):

            @pl.when(i * chunk < length)
            def _(i=i):
                w_ref[0, i] = (score[i] * inverse).astype(bf16)

    heads = per_group * kv_dev
    extra = [] if earlier is None else [earlier]
    return pl.pallas_call(
        kernel,
        grid=(seq_dev,),
        out_shape=(
            jax.ShapeDtypeStruct((seq_dev, chunks, rows, chunk), bf16),
            jax.ShapeDtypeStruct((seq_dev, rows, head_dim), f32),
            jax.ShapeDtypeStruct((kv_dev, seq_dev, context, head_dim), bf16),
        ),
        in_specs=[
            pl.BlockSpec(memory_space=pltpu.SMEM),
            pl.BlockSpec((1, rows_pad, q_cols), lambda s: (s, 0, k)),
            pl.BlockSpec((1, rows_pad, head_dim), lambda s: (s, 0, heads + k)),
            pl.BlockSpec((1, rows_pad, head_dim), lambda s: (s, 0, heads + kv_dev + k)),
            pl.BlockSpec((rows, rows_pad), lambda s: (0, 0)),
            pl.BlockSpec((senders, 1, slab, head_dim), lambda s: (0, s, 0, 0)),
        ]
        + [pl.BlockSpec(memory_space=pl.ANY)] * len(extra),
        out_specs=(
            pl.BlockSpec((1, chunks, rows, chunk), lambda s: (s, 0, 0, 0)),
            pl.BlockSpec((1, rows, head_dim), lambda s: (s, 0, 0)),
            pl.BlockSpec((1, 1, context, head_dim), lambda s: (k, s, 0, 0)),
        ),
        scratch_shapes=[
            pltpu.VMEM((rows, head_dim), bf16),
            pltpu.VMEM((chunks, rows, chunk), f32),
            pltpu.VMEM((rows, 1), f32),
            pltpu.VMEM((rows, 1), f32),
        ],
        input_output_aliases={6: 2} if extra else {},
        cost_estimate=pl.CostEstimate(flops=2_000_000_000, bytes_accessed=10_000_000, transcendentals=4_000_000),
        name="score",
    )(lengths, qkv, qkv, qkv, visible_new, k_got, *extra)


def blend_head(k, weights, new_part, lengths, hi, v_got, kv_dev, per_group, rows_pad, earlier):
    n_head = len(v_got)
    senders, seq_dev, slab, head_dim = v_got[0].shape
    chunks, rows, chunk = weights.shape[1:]
    part = senders * slab
    context = n_head * part
    q_cols = per_group * head_dim
    f32, bf16 = jnp.float32, jnp.bfloat16
    plain = (((1,), (0,)), ((), ()))

    def kernel(len_ref, at_ref, w_ref, new_ref, *refs):
        o_ref, vo_ref, acc = refs[-3:]
        length = len_ref[pl.program_id(0)]
        acc[...] = new_ref[0]
        for d in range(n_head):
            at = lax.rem(at_ref[0] + n_head - d, n_head) * part
            vo_ref[0, 0, pl.ds(pl.multiple_of(at, part), part), :] = refs[d][:, 0].reshape(part, head_dim)
        for i in range(chunks):

            @pl.when(i * chunk < length)
            def _(i=i):
                acc[...] += lax.dot_general(
                    w_ref[0, i], vo_ref[0, 0, pl.ds(i * chunk, chunk), :], plain, preferred_element_type=f32
                )

        for g in range(per_group):
            o_ref[0, :, pl.ds(g * head_dim, head_dim)] = acc[pl.ds(g * rows_pad, rows_pad), :].astype(bf16)

    extra = [] if earlier is None else list(earlier)
    return pl.pallas_call(
        kernel,
        grid=(seq_dev,),
        out_shape=(
            jax.ShapeDtypeStruct((seq_dev, rows_pad, kv_dev * q_cols), bf16),
            jax.ShapeDtypeStruct((kv_dev, seq_dev, context, head_dim), bf16),
        ),
        in_specs=[
            pl.BlockSpec(memory_space=pltpu.SMEM),
            pl.BlockSpec(memory_space=pltpu.SMEM),
            pl.BlockSpec((1, chunks, rows, chunk), lambda s: (s, 0, 0, 0)),
            pl.BlockSpec((1, rows, head_dim), lambda s: (s, 0, 0)),
        ]
        + [pl.BlockSpec((senders, 1, slab, head_dim), lambda s: (0, s, 0, 0))] * n_head
        + [pl.BlockSpec(memory_space=pl.ANY)] * len(extra),
        out_specs=(
            pl.BlockSpec((1, rows_pad, q_cols), lambda s: (s, 0, k)),
            pl.BlockSpec((1, 1, context, head_dim), lambda s: (k, s, 0, 0)),
        ),
        scratch_shapes=[pltpu.VMEM((rows, head_dim), f32)],
        input_output_aliases={4 + n_head: 0, 5 + n_head: 1} if extra else {},
        cost_estimate=pl.CostEstimate(flops=1_000_000_000, bytes_accessed=10_000_000, transcendentals=0),
        name="blend",
    )(lengths, hi.astype(jnp.int32).reshape(1), weights, new_part, *v_got, *extra)


def pack_head(cache, k, n_head):
    kv_total, seqs, slab, head_dim = cache.shape
    kv_dev = kv_total // n_head

    def kernel(in_ref, out_ref):
        out_ref[...] = in_ref[...]

    return pl.pallas_call(
        kernel,
        grid=(n_head,),
        out_shape=jax.ShapeDtypeStruct((n_head, seqs, slab, head_dim), cache.dtype),
        in_specs=[pl.BlockSpec((1, seqs, slab, head_dim), lambda h: (h * kv_dev + k, 0, 0, 0))],
        out_specs=pl.BlockSpec((1, seqs, slab, head_dim), lambda h: (h, 0, 0, 0)),
        cost_estimate=pl.CostEstimate(flops=2_000_000_000, bytes_accessed=4_000_000, transcendentals=0),
        name="pack",
    )(cache)


def pack_sequences(cache, n_batch):
    kv_total, seqs, slab, head_dim = cache.shape
    seq_dev = seqs // n_batch

    def kernel(in_ref, out_ref):
        out_ref[0] = in_ref[...]

    return pl.pallas_call(
        kernel,
        grid=(n_batch,),
        out_shape=jax.ShapeDtypeStruct((n_batch, kv_total, seq_dev, slab, head_dim), cache.dtype),
        in_specs=[pl.BlockSpec((kv_total, seq_dev, slab, head_dim), lambda b: (0, b, 0, 0))],
        out_specs=pl.BlockSpec((1, kv_total, seq_dev, slab, head_dim), lambda b: (b, 0, 0, 0, 0)),
        cost_estimate=pl.CostEstimate(flops=4_000_000_000, bytes_accessed=8_000_000, transcendentals=0),
        name="packs",
    )(cache)


def finish_rows(halves, cosine, sines, seq_dev, rows_seq, rows_pad, q_heads, kv_dev):
    head_dim = cosine.shape[-1]
    cut = halves[0].shape[1]
    width = cut + halves[1].shape[1]
    bf16 = jnp.bfloat16

    def kernel(sum_a, sum_b, cos_ref, sin_ref, out_ref):
        for s in range(seq_dev):
            c, t = cos_ref[s], sin_ref[s]
            out_ref[s, pl.ds(rows_pad - 16, 16), :] = jnp.zeros((16, width), bf16)
            rows = pl.ds(s * rows_seq, rows_seq)
            for head in range(width // head_dim):
                at = head * head_dim
                total, at = (sum_a, at) if at < cut else (sum_b, at - cut)
                x = total[rows, pl.ds(at, head_dim)]
                if head < q_heads + kv_dev:
                    x = x * c[:rows_seq] + pltpu.roll(x, head_dim // 2, 1) * t[:rows_seq]
                out_ref[s, pl.ds(0, rows_seq), pl.ds(head * head_dim, head_dim)] = x.astype(bf16)

    vmem = pl.BlockSpec(memory_space=pltpu.VMEM)
    return pl.pallas_call(
        kernel,
        out_shape=jax.ShapeDtypeStruct((seq_dev, rows_pad, width), bf16),
        in_specs=[vmem] * 4,
        out_specs=vmem,
        cost_estimate=pl.CostEstimate(flops=2_000_000_000, bytes_accessed=4_000_000, transcendentals=0),
        name="finish",
    )(*halves, cosine, sines)


def norm_pieces(sources, hi, bi, n_head, n_batch):
    rows, width = sources[0].shape
    depth = n_head * width // n_batch
    per_plane = width // depth
    f32, bf16 = jnp.float32, jnp.bfloat16

    def kernel(at_ref, *refs):
        ins = refs[: len(sources)]
        outs = refs[len(sources) : len(sources) + n_batch]
        wide, inverse = refs[-2:]
        h, b = at_ref[0], at_ref[1]
        for d in range(1 - n_head, n_head):
            p = h - d

            @pl.when(jnp.logical_and(p >= 0, p < n_head))
            def _(d=d, p=p):
                wide[p] = ins[d + n_head - 1][...]

        squares = jnp.zeros((rows, 1), f32)
        for p in range(n_head):
            x = wide[p].astype(f32)
            squares += jnp.sum(x * x, axis=-1, keepdims=True)
        inverse[...] = lax.rsqrt(squares / (n_head * width) + NORM_EPS)
        for s in range(n_batch):
            j = jnp.bitwise_xor(b, s)
            at = pl.multiple_of((j % per_plane) * depth, depth)
            outs[s][...] = (wide[j // per_plane, :, pl.ds(at, depth)].astype(f32) * inverse[...]).astype(bf16)

    vmem = pl.BlockSpec(memory_space=pltpu.VMEM)
    return pl.pallas_call(
        kernel,
        out_shape=tuple(jax.ShapeDtypeStruct((rows, depth), bf16) for _ in range(n_batch)),
        in_specs=[pl.BlockSpec(memory_space=pltpu.SMEM)] + [vmem] * len(sources),
        out_specs=(vmem,) * n_batch,
        scratch_shapes=[pltpu.VMEM((n_head, rows, width), bf16), pltpu.VMEM((rows, 1), f32)],
        cost_estimate=pl.CostEstimate(flops=2_000_000_000, bytes_accessed=8_000_000, transcendentals=0),
        name="norm",
    )(jnp.stack([hi, bi]).astype(jnp.int32), *sources)


def layer(
    window_ids,
    pool_ids,
    guess_index,
    lengths,
    embed_table,
    w_query,
    w_key,
    w_value,
    k_cache,
    v_cache,
):
    offsets, allowed = layout_tables()
    total_rows = offsets.shape[0]
    n_head = lax.axis_size("head")
    n_batch = lax.axis_size("batch")
    kv_total, seq_total, slab, head_dim = k_cache.shape
    kv_dev = kv_total // n_head
    seq_dev = seq_total // n_batch
    hi = lax.axis_index("head")
    bi = lax.axis_index("batch")
    f32 = jnp.float32

    def exchange(cache, k):
        shaped = pack_head(cache, k, n_head).reshape(n_head * n_batch, seq_dev, slab, head_dim)
        return lax.all_to_all(shaped, ("head", "batch"), split_axis=0, concat_axis=0, tiled=True)

    k_got = [exchange(k_cache, k) for k in range(kv_dev)]

    v_packed = pack_sequences(v_cache, n_batch)
    v_near = lax.all_to_all(v_packed, "batch", split_axis=0, concat_axis=0, tiled=True)
    v_near = v_near.reshape(n_batch, n_head, kv_dev, seq_dev, slab, head_dim)
    v_got = []
    for k in range(kv_dev):
        v_got.append([])
        for d in range(n_head):
            ours = lax.dynamic_index_in_dim(v_near[:, :, k], (hi + d) % n_head, 1, keepdims=False)
            shift = [(i, (i + d) % n_head) for i in range(n_head)]
            v_got[k].append(lax.ppermute(ours, "head", shift) if d else ours)

    def swap(block, step):
        return lax.ppermute(block, "batch", [(i, i ^ step) for i in range(n_batch)])

    def halve(blocks, bits, send=lambda t: t, keep=lambda t: t):
        arr = blocks
        for n, bit in enumerate(bits):
            low = 1 << sorted(bits[n:]).index(bit)
            shape = arr.shape
            arr = arr.reshape((shape[0] // (2 * low), 2, low) + shape[1:])
            out = send(arr[:, 1])
            got = swap(out, bit)
            arr = keep(arr[:, 0]) + keep(got)
            arr = arr.reshape((shape[0] // 2,) + shape[1:])
        return arr[0]

    bits = [1 << i for i in range(n_batch.bit_length() - 1)]
    rows_seq = total_rows + 1
    group_rows = seq_dev * rows_seq

    even, odd = lookup_rows(window_ids, pool_ids, guess_index, embed_table, n_batch, rows_seq)
    merged = even + swap(odd, 1)
    cut = merged.shape[-1] // 2
    mine = jnp.concatenate(
        [halve(merged[..., :cut], bits[1:]), halve(merged[..., cut:], bits[:0:-1])],
        axis=-1,
    )

    right = [(i, i + 1) for i in range(n_head - 1)]
    left = [(i + 1, i) for i in range(n_head - 1)]
    up, down = [mine], [mine]
    for _ in range(1, n_head):
        up.append(lax.ppermute(up[-1], "head", right))
        down.append(lax.ppermute(down[-1], "head", left))
    pieces = norm_pieces(down[:0:-1] + [mine] + up[1:], hi, bi, n_head, n_batch)

    parts = [pieces[0]] + [None] * (n_batch - 1)
    for step in range(n_batch - 1, 0, -1):
        parts[step] = swap(pieces[step], step)

    weights = jnp.concatenate([w_query, w_key, w_value], axis=1)

    def project(blocks):
        stacked = jnp.concatenate(blocks, axis=0)
        done = jnp.dot(stacked, weights, preferred_element_type=f32)
        return done.reshape(len(blocks), group_rows, weights.shape[1])

    narrow, widen = (lambda t: t.astype(SUM_TYPE)), (lambda t: t.astype(f32))
    odd_part = narrow(project(parts[1::2]))
    odd_got = widen(swap(odd_part, 1))
    summed = project(parts[0::2]) + odd_got
    cut = weights.shape[1] // (2 * head_dim) * head_dim
    halves = (halve(summed[..., :cut], bits[1:], narrow, widen), halve(summed[..., cut:], bits[:0:-1], narrow, widen))

    rows_pad = round_up(rows_seq, 16)
    offsets_pad = np.zeros(rows_pad, np.int32)
    offsets_pad[:total_rows] = offsets
    positions = lengths[:, None] + jnp.asarray(offsets_pad)[None, :]
    half_dim = head_dim // 2
    ladder = jnp.arange(half_dim).astype(f32)
    frequencies = jnp.power(ROPE_BASE, ladder * (-2.0 / head_dim))
    angles = positions.astype(f32)[..., None] * frequencies
    cosine = jnp.cos(angles)
    sines = jnp.sin(angles)
    cosine = jnp.concatenate([cosine, cosine], axis=-1)
    sines = jnp.concatenate([-sines, sines], axis=-1)

    per_group = w_query.shape[1] // head_dim // kv_dev
    mask = np.zeros((rows_pad, rows_pad), np.float32)
    mask[:total_rows, :total_rows] = allowed
    mask[total_rows:, 0] = 1.0
    mask = jnp.asarray(np.tile(mask, (per_group, 1)))
    qkv = finish_rows(halves, cosine, sines, seq_dev, rows_seq, rows_pad, w_query.shape[1] // head_dim, kv_dev)
    scored, k_here = [], None
    for k in range(kv_dev):
        *pair, k_here = score_head(
            k, qkv, mask, lengths, k_got[k], kv_dev, per_group, k_here
        )
        scored.append(pair)
    done = None
    for k in range(kv_dev):
        done = blend_head(k, *scored[k], lengths, hi, v_got[k], kv_dev, per_group, rows_pad, done)
    attended, v_here = done
    attended = attended[:, :total_rows].reshape(seq_dev * total_rows, w_query.shape[1])
    return (attended, k_here, v_here)


def solution(mesh):
    placed = (
        P(),
        P(),
        P(),
        P("batch"),
        P("batch", "head"),
        P("batch", "head"),
        P("batch", "head"),
        P("batch", "head"),
        P(None, None, ("head", "batch"), None),
        P(None, None, ("head", "batch"), None),
    )
    return jax.shard_map(
        layer,
        mesh=mesh,
        in_specs=placed,
        out_specs=(
            P("batch", "head"),
            P("head", "batch", None, None),
            P("head", "batch", None, None),
        ),
        check_vma=False,
    )
```
